32 devices in a mesh: dp: 2 (over core), seq: 16 (over z, y, x).
Axes of the slice: x: 2, y: 2, z: 4, core: 2. Of those that a mesh axis runs over, the one named last changes fastest.
Arguments:
- latent: bfloat16 [32, 1024, 1152], P(('dp', 'seq')), parts along dimension 0, may hold values from -6 to 6
- w_qkv_space: bfloat16 [1152, 1728], replicated, may hold values from -0.1875 to 0.1875
- w_out_space: bfloat16 [576, 1152], replicated, may hold values from -0.25 to 0.25
- w_qkv_time: bfloat16 [1152, 1728], replicated, may hold values from -0.1875 to 0.1875
- w_out_time: bfloat16 [576, 1152], replicated, may hold values from -0.25 to 0.25
- modulation: float32 [12, 1152], P('dp'), parts along dimension 0, may hold values from -1.5 to 5
Outputs:
- block_out: bfloat16 [32, 1024, 1152], P(('dp', 'seq')), parts along dimension 0
The draws below stay inside these ranges and needn't reach their ends.
There are 2 independent parts, one for each index of `dp`. The reference program is written for one: setup_inputs(seed, part) draws one part's arguments, and reference() takes and returns one part's arrays. A program takes and returns all parts, laid end to end along the dimension named above; an argument that names none is the same for every part. Nothing has to cross between parts.
All inputs are finite; a program needn't handle non-finite values.
Results may differ from the reference program's by a relative error of at most 0.02.
The reference program's roundings to bfloat16 on the way count: a program that leaves them out, or rounds other values in their place, can miss the bound.
Values may be sent and summed in bfloat16 or wider, within the bound.
No kernel may reach another device: no remote copies, remote signals or barrier semaphores. Data moves between devices by JAX's collectives and lax.ppermute only.
A program may use at most 128 MiB of HBM per device.

```python
import jax
import jax.numpy as jnp
from jax import lax

D = 1152
HEADS = 8
HEAD_DIM = 72
S = 1024
FRAMES = 16


def draw_modulation(key, part):
    key_one = jax.random.fold_in(jax.random.fold_in(key, 17), 0)
    normal = jax.random.normal(key_one, (6, D), jnp.float32) * 0.5
    return jnp.clip(normal, -1.5, 1.5)


def level_of(rng, shape, cuts, smallest, largest):
    level, own = 1.0, jax.random.fold_in(rng, 6)
    for dim, shards_of in cuts:
        draws = jnp.exp(jax.random.uniform(jax.random.fold_in(own, dim), (shards_of,), jnp.float32, smallest / len(cuts), largest / len(cuts)))
        level = level * jnp.repeat(draws, shape[dim] // shards_of).reshape([-1 if axis == dim else 1 for axis in range(len(shape))])
    return level


def bell_draw(own_key, extent, scale, reach, shards=(), kind=jnp.bfloat16):
    array = scale * jax.random.normal(own_key, extent, jnp.float32)
    if shards:
        array = array * level_of(own_key, extent, shards, -0.22, 0.18)
    return jnp.clip(array, -reach, reach).astype(kind)


def setup_inputs(seed: int = 0, part: int = 0) -> dict:
    seeds = jax.random.split(jax.random.key(seed), 7)
    part_keys = jax.random.split(jax.random.fold_in(seeds[6], part), 7)
    latent = bell_draw(part_keys[0], (FRAMES, S, D), 1.0, 6.0, ((0, 16),))
    w_qkv_space = bell_draw(seeds[1], (D, 3 * HEADS * HEAD_DIM), D ** -0.5, 0.1875)
    w_out_space = bell_draw(seeds[2], (HEADS * HEAD_DIM, D), (HEADS * HEAD_DIM) ** -0.5, 0.25)
    w_qkv_time = bell_draw(seeds[3], (D, 3 * HEADS * HEAD_DIM), D ** -0.5, 0.1875)
    w_out_time = bell_draw(seeds[4], (HEADS * HEAD_DIM, D), (HEADS * HEAD_DIM) ** -0.5, 0.25)
    modulation = draw_modulation(jax.random.fold_in(jax.random.fold_in(seeds[6], part), 71), part)
    return {"latent": latent, "w_qkv_space": w_qkv_space, "w_out_space": w_out_space, "w_qkv_time": w_qkv_time, "w_out_time": w_out_time, "modulation": modulation}


EPS = 1e-06

def normalize(values):
    center = lax.optimization_barrier(jnp.mean(values, -1, keepdims=True))
    centred = values - center
    spread = lax.optimization_barrier(jnp.mean(centred * centred, -1, keepdims=True))
    return centred * lax.rsqrt(spread + EPS)

def modulated(latent, modulation, first):
    normed = normalize(latent.astype(jnp.float32))
    return (normed * (1.0 + modulation[first + 1]) + modulation[first]).astype(jnp.bfloat16)

def softmax_weights(scores, axis):
    top_score = lax.optimization_barrier(jnp.max(scores, axis, keepdims=True))
    expo = jnp.exp(scores - top_score)
    return (expo / lax.optimization_barrier(jnp.sum(expo, axis, keepdims=True))).astype(jnp.bfloat16)

def attend_space(frame_rows, w_qkv, w_out, modulation):
    tokens_here = frame_rows.shape[0]
    mixed = modulated(frame_rows, modulation, 0)
    triple = jnp.dot(mixed, w_qkv, preferred_element_type=jnp.float32).astype(jnp.bfloat16)
    triple = triple.reshape(tokens_here, 3, HEADS, HEAD_DIM).astype(jnp.float32)
    factor = 1.0 / math_sqrt(HEAD_DIM)
    scores = jnp.einsum('shd,thd->hst', triple[:, 0], triple[:, 1]) * factor
    weights = softmax_weights(scores, 2).astype(jnp.float32)
    outputs = jnp.einsum('hst,thd->shd', weights, triple[:, 2]).astype(jnp.bfloat16)
    delta = jnp.dot(outputs.reshape(tokens_here, HEADS * HEAD_DIM), w_out, preferred_element_type=jnp.float32)
    return (frame_rows.astype(jnp.float32) + modulation[2] * delta).astype(jnp.bfloat16)

def math_sqrt(value):
    return float(value) ** 0.5

def attend_time(queries, key_heads, value_heads):
    factor = 1.0 / math_sqrt(queries.shape[-1])
    scores = jnp.einsum('fphd,gphd->phfg', queries.astype(jnp.float32), key_heads.astype(jnp.float32)) * factor
    weights = softmax_weights(scores, 3).astype(jnp.float32)
    return jnp.einsum('phfg,gphd->fphd', weights, value_heads.astype(jnp.float32)).astype(jnp.bfloat16)

def reference(latent, w_qkv_space, w_out_space, w_qkv_time, w_out_time, modulation):
    after_space = lax.map(lambda one_frame: attend_space(one_frame, w_qkv_space, w_out_space, modulation), latent)
    frames, spatial, width = after_space.shape
    mixed = modulated(after_space, modulation, 3).reshape(frames * spatial, width)
    triple = jnp.dot(mixed, w_qkv_time, preferred_element_type=jnp.float32).astype(jnp.bfloat16)
    triple = triple.reshape(frames, spatial, 3, HEADS, HEAD_DIM)
    outputs = attend_time(triple[:, :, 0], triple[:, :, 1], triple[:, :, 2])
    delta = jnp.dot(outputs.reshape(frames * spatial, HEADS * HEAD_DIM), w_out_time, preferred_element_type=jnp.float32)
    result = after_space.astype(jnp.float32).reshape(frames * spatial, width) + modulation[5] * delta
    return result.astype(jnp.bfloat16).reshape(frames, spatial, width)
```

```python
import functools
import math

import jax
import jax.numpy as jnp
from jax import lax
from jax.experimental import pallas as pl
from jax.experimental.pallas import tpu as pltpu
from jax.sharding import PartitionSpec as P

HEADS = 8
HEAD_DIM = 72
EPS = 1e-06
CHUNKS = 4
INNER = HEADS * HEAD_DIM
POWER = math.log2(math.e) / math.sqrt(HEAD_DIM)
LIMIT = 30 * 1024 * 1024


def mixed_rows(rows, modulation, first):
    values = rows.astype(jnp.float32)
    centred = values - jnp.mean(values, -1, keepdims=True)
    spread = jnp.mean(centred * centred, -1, keepdims=True)
    normed = centred * lax.rsqrt(spread + EPS)
    return (normed * (1.0 + modulation[first + 1]) + modulation[first]).astype(jnp.bfloat16)


def project_kernel(rows_ref, w_ref, mod_ref, out_ref):
    mixed = mixed_rows(rows_ref[...], mod_ref[...], 0)
    out_ref[...] = jnp.dot(mixed, w_ref[...], preferred_element_type=jnp.float32).astype(jnp.bfloat16)


def attend(query, key, value, keep=None):
    scores = lax.dot_general(query, key, (((1,), (1,)), ((), ())), preferred_element_type=jnp.float32)
    if keep is not None:
        scores = jnp.where(keep, scores, -jnp.inf)
    top = jnp.max(scores, 1, keepdims=True)
    expo = jnp.exp2((scores - top) * POWER)
    total = jnp.sum(expo, 1, keepdims=True)
    out = jnp.dot(expo.astype(jnp.bfloat16), value, preferred_element_type=jnp.float32)
    return (out / total).astype(jnp.bfloat16)


def head_columns(kind, head):
    start = kind * INNER + head * HEAD_DIM
    return slice(start, start + HEAD_DIM)


def space_kernel(rows_ref, query_ref, triple_ref, w_out_ref, mod_ref, out_ref, heads_ref):
    for head in range(HEADS):
        heads_ref[:, head_columns(0, head)] = attend(
            query_ref[:, head_columns(0, head)],
            triple_ref[:, head_columns(1, head)],
            triple_ref[:, head_columns(2, head)],
        )
    delta = jnp.dot(heads_ref[...], w_out_ref[...], preferred_element_type=jnp.float32)
    out_ref[...] = (rows_ref[...].astype(jnp.float32) + mod_ref[2] * delta).astype(jnp.bfloat16)


def time_kernel(rows_ref, w_ref, mod_ref, out_ref, triple_ref, *, positions):
    mixed = mixed_rows(rows_ref[...], mod_ref[...], 3)
    triple_ref[...] = jnp.dot(mixed, w_ref[...], preferred_element_type=jnp.float32).astype(jnp.bfloat16)
    tokens = rows_ref.shape[0]
    left = lax.broadcasted_iota(jnp.int32, (tokens, tokens), 0)
    right = lax.broadcasted_iota(jnp.int32, (tokens, tokens), 1)
    keep = lax.rem(left, positions) == lax.rem(right, positions)
    for head in range(HEADS):
        out_ref[:, head_columns(0, head)] = attend(
            triple_ref[:, head_columns(0, head)],
            triple_ref[:, head_columns(1, head)],
            triple_ref[:, head_columns(2, head)],
            keep,
        )


def finish_kernel(rows_ref, heads_ref, w_out_ref, mod_ref, out_ref):
    delta = jnp.dot(heads_ref[...], w_out_ref[...], preferred_element_type=jnp.float32)
    out_ref[...] = (rows_ref[...].astype(jnp.float32) + mod_ref[5] * delta).astype(jnp.bfloat16)


def whole(array):
    return pl.BlockSpec(array.shape, lambda i: (0,) * array.ndim)


def project(frame, w_qkv, modulation, steps):
    tokens, width = frame.shape
    block = tokens // steps
    return pl.pallas_call(
        project_kernel,
        grid=(steps,),
        in_specs=[pl.BlockSpec((block, width), lambda i: (i, 0)), whole(w_qkv), whole(modulation)],
        out_specs=pl.BlockSpec((block, w_qkv.shape[1]), lambda i: (i, 0)),
        out_shape=jax.ShapeDtypeStruct((tokens, w_qkv.shape[1]), jnp.bfloat16),
        compiler_params=pltpu.CompilerParams(vmem_limit_bytes=LIMIT),
        cost_estimate=pl.CostEstimate(flops=2 * tokens * width * w_qkv.shape[1], transcendentals=0, bytes_accessed=10000000),
        name="project",
    )(frame, w_qkv, modulation)


def space_chunk(frame, triple, w_out, modulation, chunk):
    tokens, width = frame.shape
    block = tokens // CHUNKS
    return pl.pallas_call(
        space_kernel,
        grid=(1,),
        in_specs=[
            pl.BlockSpec((block, width), lambda i: (chunk, 0)),
            pl.BlockSpec((block, triple.shape[1]), lambda i: (chunk, 0)),
            whole(triple),
            whole(w_out),
            whole(modulation),
        ],
        out_specs=pl.BlockSpec((block, width), lambda i: (0, 0)),
        out_shape=jax.ShapeDtypeStruct((block, width), jnp.bfloat16),
        scratch_shapes=[pltpu.VMEM((block, INNER), jnp.bfloat16)],
        compiler_params=pltpu.CompilerParams(vmem_limit_bytes=LIMIT),
        cost_estimate=pl.CostEstimate(flops=6 * block * tokens * 256 * HEADS, transcendentals=HEADS * block * tokens, bytes_accessed=6000000),
        name="space",
    )(frame, triple, triple, w_out, modulation)


def time_chunk(patches, w_qkv, modulation, members):
    tokens, width = patches.shape
    return pl.pallas_call(
        functools.partial(time_kernel, positions=tokens // members),
        grid=(1,),
        in_specs=[whole(patches), whole(w_qkv), whole(modulation)],
        out_specs=pl.BlockSpec((tokens, INNER), lambda i: (0, 0)),
        out_shape=jax.ShapeDtypeStruct((tokens, INNER), jnp.bfloat16),
        scratch_shapes=[pltpu.VMEM((tokens, w_qkv.shape[1]), jnp.bfloat16)],
        compiler_params=pltpu.CompilerParams(vmem_limit_bytes=LIMIT),
        cost_estimate=pl.CostEstimate(flops=4 * tokens * width * w_qkv.shape[1], transcendentals=HEADS * tokens * tokens, bytes_accessed=5000000),
        name="time",
    )(patches, w_qkv, modulation)


def finish_all(rows, heads, w_out, modulation):
    count = len(rows)
    block, width = rows[0].shape
    tokens = count * block

    def kernel(*refs):
        w_ref, mod_ref, out_ref = refs[2 * count :]
        for index in range(count):
            delta = jnp.dot(refs[count + index][...], w_ref[...], preferred_element_type=jnp.float32)
            done = refs[index][...].astype(jnp.float32) + mod_ref[5] * delta
            out_ref[index * block : (index + 1) * block] = done.astype(jnp.bfloat16)

    return pl.pallas_call(
        kernel,
        out_shape=jax.ShapeDtypeStruct((tokens, width), jnp.bfloat16),
        compiler_params=pltpu.CompilerParams(vmem_limit_bytes=LIMIT),
        cost_estimate=pl.CostEstimate(flops=2 * tokens * width * INNER, transcendentals=0, bytes_accessed=7000000),
        name="finish",
    )(*rows, *heads, w_out, modulation)


def exchange(array):
    return lax.all_to_all(array, "seq", split_axis=0, concat_axis=0, tiled=True)


def shards(latent, w_qkv_space, w_out_space, w_qkv_time, w_out_time, modulation):
    members = lax.axis_size("seq")
    frame = latent[0]
    triple = project(frame, w_qkv_space, modulation, 4)
    rows = [space_chunk(frame, triple, w_out_space, modulation, chunk) for chunk in range(CHUNKS)]
    patches = [exchange(part) for part in rows]
    heads = [exchange(time_chunk(part, w_qkv_time, modulation, members)) for part in patches]
    return finish_all(rows, heads, w_out_time, modulation)[None]


def solution(mesh):
    in_specs = (P(("dp", "seq"), None, None), P(), P(), P(), P(), P("dp", None))
    out_specs = P(("dp", "seq"), None, None)
    return jax.shard_map(shards, mesh=mesh, in_specs=in_specs, out_specs=out_specs, check_vma=False)
```

```python
import functools
import math

import jax
import jax.numpy as jnp
from jax import lax
from jax.experimental import pallas as pl
from jax.experimental.pallas import tpu as pltpu
from jax.sharding import PartitionSpec as P

HEADS = 8
HEAD_DIM = 72
EPS = 1e-06
CHUNKS = 2
ROWS = 256
INNER = HEADS * HEAD_DIM
POWER = math.log2(math.e) / math.sqrt(HEAD_DIM)
LIMIT = 20 * 1024 * 1024


def mixed_rows(rows, modulation, first):
    values = rows.astype(jnp.float32)
    centred = values - jnp.mean(values, -1, keepdims=True)
    spread = jnp.mean(centred * centred, -1, keepdims=True)
    normed = centred * lax.rsqrt(spread + EPS)
    return (normed * (1.0 + modulation[first + 1]) + modulation[first]).astype(jnp.bfloat16)


def rows_by_columns(rows, w_t):
    product = lax.dot_general(rows, w_t, (((1,), (1,)), ((), ())), preferred_element_type=jnp.float32)
    return product.astype(jnp.bfloat16)


def project_kernel(rows_ref, w_ref, mod_ref, out_ref):
    mixed = mixed_rows(rows_ref[...], mod_ref[...], 0)
    out_ref[...] = rows_by_columns(mixed, w_ref[...])


def attend(query, key, value, keep=None):
    scores = lax.dot_general(query, key, (((1,), (1,)), ((), ())), preferred_element_type=jnp.float32)
    if keep is not None:
        scores = jnp.where(keep, scores, -jnp.inf)
    top = jnp.max(scores, 1, keepdims=True)
    expo = jnp.exp2((scores - top) * POWER)
    total = jnp.sum(expo, 1, keepdims=True)
    out = jnp.dot(expo.astype(jnp.bfloat16), value, preferred_element_type=jnp.float32)
    return (out / total).astype(jnp.bfloat16)


def head_columns(kind, head):
    start = kind * INNER + head * HEAD_DIM
    return slice(start, start + HEAD_DIM)


def space_kernel(rows_ref, query_ref, triple_ref, w_out_ref, mod_ref, out_ref, heads_ref):
    for head in range(HEADS):
        heads_ref[:, head_columns(0, head)] = attend(
            query_ref[:, head_columns(0, head)],
            triple_ref[:, head_columns(1, head)],
            triple_ref[:, head_columns(2, head)],
        )
    delta = jnp.dot(heads_ref[...], w_out_ref[...], preferred_element_type=jnp.float32)
    out_ref[...] = (rows_ref[...].astype(jnp.float32) + mod_ref[2] * delta).astype(jnp.bfloat16)


def time_kernel(rows_ref, w_ref, mod_ref, out_ref, triple_ref, heads_ref):
    members, positions, width = rows_ref.shape
    tokens = members * positions
    rows = rows_ref[...].astype(jnp.float32).reshape(tokens, width)
    triple_ref[...] = rows_by_columns(mixed_rows(rows, mod_ref[...], 3), w_ref[...])
    left = lax.broadcasted_iota(jnp.int32, (tokens, tokens), 0)
    right = lax.broadcasted_iota(jnp.int32, (tokens, tokens), 1)
    keep = lax.rem(left, positions) == lax.rem(right, positions)
    for head in range(HEADS):
        heads_ref[:, head_columns(0, head)] = attend(
            triple_ref[:, head_columns(0, head)],
            triple_ref[:, head_columns(1, head)],
            triple_ref[:, head_columns(2, head)],
            keep,
        )
    done = heads_ref[...].astype(jnp.float32).reshape(members, positions, INNER)
    out_ref[...] = done.astype(jnp.bfloat16)


def finish_kernel(rows_ref, heads_ref, w_out_ref, mod_ref, *refs):
    delta = jnp.dot(heads_ref[...], w_out_ref[...], preferred_element_type=jnp.float32)
    refs[-1][...] = (rows_ref[...].astype(jnp.float32) + mod_ref[5] * delta).astype(jnp.bfloat16)


def whole(array):
    return pl.BlockSpec(array.shape, lambda i: (0,) * array.ndim)


def params():
    return pltpu.CompilerParams(vmem_limit_bytes=LIMIT)


def project(frame, w_t, modulation):
    tokens, width = frame.shape
    columns = w_t.shape[0]
    return pl.pallas_call(
        project_kernel,
        grid=(tokens // ROWS,),
        in_specs=[pl.BlockSpec((ROWS, width), lambda i: (i, 0)), whole(w_t), whole(modulation)],
        out_specs=pl.BlockSpec((ROWS, columns), lambda i: (i, 0)),
        out_shape=jax.ShapeDtypeStruct((tokens, columns), jnp.bfloat16),
        compiler_params=params(),
        cost_estimate=pl.CostEstimate(flops=2 * tokens * width * columns, transcendentals=0, bytes_accessed=10000000),
        name="project",
    )(frame, w_t, modulation)


def space_chunk(frame, triple, w_out, modulation, chunk):
    tokens, width = frame.shape
    block = tokens // CHUNKS
    steps = block // ROWS
    return pl.pallas_call(
        space_kernel,
        grid=(steps,),
        in_specs=[
            pl.BlockSpec((ROWS, width), lambda i: (chunk * steps + i, 0)),
            pl.BlockSpec((ROWS, triple.shape[1]), lambda i: (chunk * steps + i, 0)),
            whole(triple),
            whole(w_out),
            whole(modulation),
        ],
        out_specs=pl.BlockSpec((ROWS, width), lambda i: (i, 0)),
        out_shape=jax.ShapeDtypeStruct((block, width), jnp.bfloat16),
        scratch_shapes=[pltpu.VMEM((ROWS, INNER), jnp.bfloat16)],
        compiler_params=params(),
        cost_estimate=pl.CostEstimate(flops=6 * block * tokens * 256 * HEADS, transcendentals=HEADS * block * tokens, bytes_accessed=6000000),
        name="space",
    )(frame, triple, triple, w_out, modulation)


def time_chunk(patches, w_t, modulation, members):
    tokens, width = patches.shape
    positions = tokens // members
    some = min(positions, max(8, ROWS // members))
    columns = w_t.shape[0]
    heads = pl.pallas_call(
        time_kernel,
        grid=(positions // some,),
        in_specs=[pl.BlockSpec((members, some, width), lambda i: (0, i, 0)), whole(w_t), whole(modulation)],
        out_specs=pl.BlockSpec((members, some, INNER), lambda i: (0, i, 0)),
        out_shape=jax.ShapeDtypeStruct((members, positions, INNER), jnp.bfloat16),
        scratch_shapes=[pltpu.VMEM((members * some, columns), jnp.bfloat16), pltpu.VMEM((members * some, INNER), jnp.bfloat16)],
        compiler_params=params(),
        cost_estimate=pl.CostEstimate(flops=4 * tokens * width * columns, transcendentals=HEADS * tokens * tokens, bytes_accessed=5000000),
        name="time",
    )(patches.reshape(members, positions, width), w_t, modulation)
    return heads.reshape(tokens, INNER)


def finish_chunk(rows, heads, w_out, modulation, chunk, earlier):
    block, width = rows.shape
    steps = block // ROWS
    extra = [] if earlier is None else [earlier]
    return pl.pallas_call(
        finish_kernel,
        grid=(steps,),
        in_specs=[
            pl.BlockSpec((ROWS, width), lambda i: (i, 0)),
            pl.BlockSpec((ROWS, INNER), lambda i: (i, 0)),
            whole(w_out),
            whole(modulation),
        ]
        + [pl.BlockSpec(memory_space=pl.ANY) for _ in extra],
        out_specs=pl.BlockSpec((ROWS, width), lambda i: (chunk * steps + i, 0)),
        out_shape=jax.ShapeDtypeStruct((block * CHUNKS, width), jnp.bfloat16),
        input_output_aliases={4: 0} if extra else {},
        compiler_params=params(),
        cost_estimate=pl.CostEstimate(flops=2 * block * width * INNER, transcendentals=0, bytes_accessed=4000000),
        name="finish",
    )(rows, heads, w_out, modulation, *extra)


def exchange(array):
    return lax.all_to_all(array, "seq", split_axis=0, concat_axis=0, tiled=True)


def shards(latent, w_qkv_space, w_out_space, w_qkv_time, w_out_time, modulation):
    members = lax.axis_size("seq")
    frame = latent[0]
    triple = project(frame, w_qkv_space.T, modulation)
    rows = [space_chunk(frame, triple, w_out_space, modulation, chunk) for chunk in range(CHUNKS)]
    patches = [exchange(part) for part in rows]
    heads = [exchange(time_chunk(part, w_qkv_time.T, modulation, members)) for part in patches]
    done = None
    for chunk in range(CHUNKS):
        done = finish_chunk(rows[chunk], heads[chunk], w_out_time, modulation, chunk, done)
    return done[None]


def solution(mesh):
    in_specs = (P(("dp", "seq"), None, None), P(), P(), P(), P(), P("dp", None))
    out_specs = P(("dp", "seq"), None, None)
    return jax.shard_map(shards, mesh=mesh, in_specs=in_specs, out_specs=out_specs, check_vma=False)
```

```python
import functools
import math

import jax
import jax.numpy as jnp
from jax import lax
from jax.experimental import pallas as pl
from jax.experimental.pallas import tpu as pltpu
from jax.sharding import PartitionSpec as P

HEADS = 8
HEAD_DIM = 72
EPS = 1e-06
CHUNKS = 2
ROWS = 256
INNER = HEADS * HEAD_DIM
POWER = math.log2(math.e) / math.sqrt(HEAD_DIM)
LIMIT = 20 * 1024 * 1024


def mixed_rows(rows, modulation, first):
    values = rows.astype(jnp.float32)
    centred = values - jnp.mean(values, -1, keepdims=True)
    spread = jnp.mean(centred * centred, -1, keepdims=True)
    normed = centred * lax.rsqrt(spread + EPS)
    return (normed * (1.0 + modulation[first + 1]) + modulation[first]).astype(jnp.bfloat16)


def rows_by_columns(rows, w_t):
    product = lax.dot_general(rows, w_t, (((1,), (1,)), ((), ())), preferred_element_type=jnp.float32)
    return product.astype(jnp.bfloat16)


def project_kernel(rows_ref, w_ref, mod_ref, out_ref):
    mixed = mixed_rows(rows_ref[...], mod_ref[...], 0)
    out_ref[...] = rows_by_columns(mixed, w_ref[...])


def attend(query, key, value, keep=None):
    scores = lax.dot_general(query, key, (((1,), (1,)), ((), ())), preferred_element_type=jnp.float32)
    if keep is not None:
        scores = jnp.where(keep, scores, -jnp.inf)
    top = jnp.max(scores, 1, keepdims=True)
    expo = jnp.exp2((scores - top) * POWER)
    total = jnp.sum(expo, 1, keepdims=True)
    out = jnp.dot(expo.astype(jnp.bfloat16), value, preferred_element_type=jnp.float32)
    return (out / total).astype(jnp.bfloat16)


def head_columns(kind, head):
    start = kind * INNER + head * HEAD_DIM
    return slice(start, start + HEAD_DIM)


def space_kernel(rows_ref, query_ref, triple_ref, w_out_ref, mod_ref, out_ref, heads_ref):
    for head in range(HEADS):
        heads_ref[:, head_columns(0, head)] = attend(
            query_ref[:, head_columns(0, head)],
            triple_ref[:, head_columns(1, head)],
            triple_ref[:, head_columns(2, head)],
        )
    out_ref[...] = gated(rows_ref[...], heads_ref[...], w_out_ref[...], mod_ref[2])


def gated(rows, heads, w_out, gate):
    delta = jnp.dot(heads, w_out, preferred_element_type=jnp.float32)
    return (rows.astype(jnp.float32) + gate * delta).astype(jnp.bfloat16)


def time_kernel(rows_ref, w_ref, mod_ref, *refs):
    out_ref, triple_ref, heads_ref = refs[-3:]
    members, positions, width = rows_ref.shape
    tokens = members * positions
    rows = rows_ref[...].astype(jnp.float32).reshape(tokens, width)
    if len(refs) > 3:
        heads = refs[0][...].astype(jnp.float32).reshape(tokens, INNER).astype(jnp.bfloat16)
        rows = gated(rows, heads, refs[1][...], mod_ref[2])
    triple_ref[...] = rows_by_columns(mixed_rows(rows, mod_ref[...], 3), w_ref[...])
    left = lax.broadcasted_iota(jnp.int32, (tokens, tokens), 0)
    right = lax.broadcasted_iota(jnp.int32, (tokens, tokens), 1)
    keep = lax.rem(left, positions) == lax.rem(right, positions)
    for head in range(HEADS):
        heads_ref[:, head_columns(0, head)] = attend(
            triple_ref[:, head_columns(0, head)],
            triple_ref[:, head_columns(1, head)],
            triple_ref[:, head_columns(2, head)],
            keep,
        )
    done = heads_ref[...].astype(jnp.float32).reshape(members, positions, INNER)
    out_ref[...] = done.astype(jnp.bfloat16)


def finish_kernel(rows_ref, heads_ref, w_out_ref, mod_ref, *refs):
    refs[-1][...] = gated(rows_ref[...], heads_ref[...], w_out_ref[...], mod_ref[5])


def whole(array):
    return pl.BlockSpec(array.shape, lambda i: (0,) * array.ndim)


def params():
    return pltpu.CompilerParams(vmem_limit_bytes=LIMIT)


def project(frame, w_t, modulation):
    tokens, width = frame.shape
    columns = w_t.shape[0]
    return pl.pallas_call(
        project_kernel,
        grid=(tokens // ROWS,),
        in_specs=[pl.BlockSpec((ROWS, width), lambda i: (i, 0)), whole(w_t), whole(modulation)],
        out_specs=pl.BlockSpec((ROWS, columns), lambda i: (i, 0)),
        out_shape=jax.ShapeDtypeStruct((tokens, columns), jnp.bfloat16),
        compiler_params=params(),
        cost_estimate=pl.CostEstimate(flops=2 * tokens * width * columns, transcendentals=0, bytes_accessed=10000000),
        name="project",
    )(frame, w_t, modulation)


def space_chunk(frame, triple, w_out, modulation, chunk):
    tokens, width = frame.shape
    block = tokens // CHUNKS
    steps = block // ROWS
    return pl.pallas_call(
        space_kernel,
        grid=(steps,),
        in_specs=[
            pl.BlockSpec((ROWS, width), lambda i: (chunk * steps + i, 0)),
            pl.BlockSpec((ROWS, triple.shape[1]), lambda i: (chunk * steps + i, 0)),
            whole(triple),
            whole(w_out),
            whole(modulation),
        ],
        out_specs=[pl.BlockSpec((ROWS, width), lambda i: (i, 0)), pl.BlockSpec((ROWS, INNER), lambda i: (i, 0))],
        out_shape=[
            jax.ShapeDtypeStruct((block, width), jnp.bfloat16),
            jax.ShapeDtypeStruct((block, INNER), jnp.bfloat16),
        ],
        compiler_params=params(),
        cost_estimate=pl.CostEstimate(flops=6 * block * tokens * 256 * HEADS, transcendentals=HEADS * block * tokens, bytes_accessed=6000000),
        name="space",
    )(frame, triple, triple, w_out, modulation)


def time_chunk(patches, w_t, modulation, members, heads_in=None, w_out=None):
    tokens, width = patches.shape
    positions = tokens // members
    some = min(positions, max(8, ROWS // members))
    columns = w_t.shape[0]
    more, specs = [], []
    if heads_in is not None:
        more = [heads_in.reshape(members, positions, INNER), w_out]
        specs = [pl.BlockSpec((members, some, INNER), lambda i: (0, i, 0)), whole(w_out)]
    heads = pl.pallas_call(
        time_kernel,
        grid=(positions // some,),
        in_specs=[pl.BlockSpec((members, some, width), lambda i: (0, i, 0)), whole(w_t), whole(modulation)] + specs,
        out_specs=pl.BlockSpec((members, some, INNER), lambda i: (0, i, 0)),
        out_shape=jax.ShapeDtypeStruct((members, positions, INNER), jnp.bfloat16),
        scratch_shapes=[pltpu.VMEM((members * some, columns), jnp.bfloat16), pltpu.VMEM((members * some, INNER), jnp.bfloat16)],
        compiler_params=params(),
        cost_estimate=pl.CostEstimate(flops=4 * tokens * width * columns, transcendentals=HEADS * tokens * tokens, bytes_accessed=5000000),
        name="time",
    )(patches.reshape(members, positions, width), w_t, modulation, *more)
    return heads.reshape(tokens, INNER)


def finish_chunk(rows, heads, w_out, modulation, chunk, earlier):
    block, width = rows.shape
    steps = block // ROWS
    extra = [] if earlier is None else [earlier]
    return pl.pallas_call(
        finish_kernel,
        grid=(steps,),
        in_specs=[
            pl.BlockSpec((ROWS, width), lambda i: (i, 0)),
            pl.BlockSpec((ROWS, INNER), lambda i: (i, 0)),
            whole(w_out),
            whole(modulation),
        ]
        + [pl.BlockSpec(memory_space=pl.ANY) for _ in extra],
        out_specs=pl.BlockSpec((ROWS, width), lambda i: (chunk * steps + i, 0)),
        out_shape=jax.ShapeDtypeStruct((block * CHUNKS, width), jnp.bfloat16),
        input_output_aliases={4: 0} if extra else {},
        compiler_params=params(),
        cost_estimate=pl.CostEstimate(flops=2 * block * width * INNER, transcendentals=0, bytes_accessed=4000000),
        name="finish",
    )(rows, heads, w_out, modulation, *extra)


def exchange(array):
    return lax.all_to_all(array, "seq", split_axis=0, concat_axis=0, tiled=True)


def shards(latent, w_qkv_space, w_out_space, w_qkv_time, w_out_time, modulation):
    members = lax.axis_size("seq")
    frame = latent[0]
    early = exchange(frame[frame.shape[0] // CHUNKS :])
    triple = project(frame, w_qkv_space.T, modulation)
    first, _ = space_chunk(frame, triple, w_out_space, modulation, 0)
    first, early = lax.optimization_barrier((first, early))
    patches = exchange(first)
    second, heads = space_chunk(frame, triple, w_out_space, modulation, 1)
    heads = exchange(heads)
    first_back = exchange(time_chunk(patches, w_qkv_time.T, modulation, members))
    second_back = exchange(time_chunk(early, w_qkv_time.T, modulation, members, heads, w_out_space))
    done = finish_chunk(first, first_back, w_out_time, modulation, 0, None)
    done = finish_chunk(second, second_back, w_out_time, modulation, 1, done)
    return done[None]


def solution(mesh):
    in_specs = (P(("dp", "seq"), None, None), P(), P(), P(), P(), P("dp", None))
    out_specs = P(("dp", "seq"), None, None)
    return jax.shard_map(shards, mesh=mesh, in_specs=in_specs, out_specs=out_specs, check_vma=False)
```
